32 devices in a mesh: req: 8 (over z, core), blk: 4 (over y, x).
Axes of the slice: x: 2, y: 2, z: 4, core: 2. Of those that a mesh axis runs over, the one named last changes fastest.
Arguments:
- draft_node_queries: bfloat16 [256, 4096], P(('req', 'blk')), parts along dimension 0, may hold values from -6 to 6, as said below
- draft_node_keys: bfloat16 [256, 512], P(('req', 'blk')), parts along dimension 0, may hold values from -6 to 6
- draft_node_values: bfloat16 [256, 512], P(('req', 'blk')), parts along dimension 0, may hold values from -6 to 6
- paged_key_cache: bfloat16 [16384, 512], P(('req', 'blk')), parts along dimension 0, may hold values from -6 to 6
- paged_value_cache: bfloat16 [16384, 512], P(('req', 'blk')), parts along dimension 0, may hold values from -6 to 6
- context_length: int32 [8], P('req'), parts along dimension 0, may hold values from 1024 to 2048
- parents: int32 [256], P('req'), parts along dimension 0, may hold values from 0 to 31, as said below
- accepted_path: int32 [64], P('req'), parts along dimension 0, may hold values from 0 to 31, as said below
- out_weight: bfloat16 [2880, 4096], P('blk'), may hold values from -0.09375 to 0.09375
Outputs:
- tree_attention: bfloat16 [256, 4096], P(('req', 'blk')), parts along dimension 0
- path_output: bfloat16 [64, 2880], P('req', 'blk'), parts along dimension 0
The draws below stay inside these ranges and needn't reach their ends.
There are 8 independent parts, one for each index of `req`. The reference program is written for one: setup_inputs(seed, part) draws one part's arguments, and reference() takes and returns one part's arrays. A program takes and returns all parts, laid end to end along the dimension named above; an argument that names none is the same for every part. Nothing has to cross between parts.
Inputs may be any that keep to these rules, and one draw needn't show every extreme that they name: `draft_node_queries`: query entries lie within the range. parents[0] = 0 marks the root; for i >= 1, parents[i] is one of the nodes i - 4 to i - 1 (and at least 0). `accepted_path`: distinct nodes; each entry after the first is a child of the one before it.
All inputs are finite; a program needn't handle non-finite values.
Results may differ from the reference program's by a relative error of at most 0.0095.
Values may be sent and summed in bfloat16 or wider, within the bound.
A program may use at most 64 MiB of HBM per device.

```python
import jax
import jax.numpy as jnp
from jax import lax

D = 2880
QUERY_HEADS = 64
KEY_VALUE_HEADS = 8
HEAD_WIDTH = 64
TREE_NODES = 32
PATH = 8
CACHED_LENGTH = 2048


def tree_links(key):
    window = TREE_NODES // 8
    indices = jnp.arange(TREE_NODES, dtype=jnp.int32)
    lowest = jnp.maximum(indices - window, 0)
    spread = jnp.maximum(indices - lowest, 1)
    offsets = jax.random.randint(jax.random.fold_in(key, 31), (TREE_NODES,), 0, 1 << 20, dtype=jnp.int32)
    linked = lowest + offsets % spread
    return jnp.where(indices == 0, 0, linked).astype(jnp.int32)


def draw_parents(key, part):
    return tree_links(key)


def draw_accepted_path(key, part):
    linked = tree_links(key)
    window = TREE_NODES // 8
    leaf_node = TREE_NODES - 1 - jax.random.randint(jax.random.fold_in(key, 32), (), 0, window, dtype=jnp.int32)
    walked = [leaf_node]
    for stepper in range(PATH - 1):
        walked.append(linked[walked[-1]])
    return jnp.stack(walked[::-1]).astype(jnp.int32)


def draw_draft_node_queries(key, part):
    base_offset = jax.random.normal(jax.random.fold_in(key, 11), (TREE_NODES, QUERY_HEADS * HEAD_WIDTH), jnp.float32)
    return jnp.clip(2.5 * base_offset, -6.0, 6.0).astype(jnp.bfloat16)


def draw_paged_key_cache(key, part):
    base_offset = jax.random.normal(jax.random.fold_in(key, 22), (CACHED_LENGTH, KEY_VALUE_HEADS * HEAD_WIDTH), jnp.float32)
    return jnp.clip(base_offset, -6.0, 6.0).astype(jnp.bfloat16)


def block_levels(key, shape, shards, smallest, high):
    def one(axis_at, shards_of):
        steps = jax.random.uniform(jax.random.fold_in(jax.random.fold_in(key, 6), axis_at), (shards_of,), jnp.float32, smallest / len(shards), high / len(shards))
        return jnp.repeat(jnp.exp(steps), shape[axis_at] // shards_of).reshape((-1,) + (1,) * (len(shape) - axis_at - 1))

    level = one(*shards[0])
    for cut in shards[1:]:
        level = level * one(*cut)
    return level


def bell_draw(stream_key, dims, scale, reach, split=(), kind=jnp.bfloat16):
    array = jax.random.normal(stream_key, dims, jnp.float32) * scale
    if len(split) > 0:
        array = block_levels(stream_key, dims, split, -0.22, 0.18) * array
    return jnp.clip(array, min=-reach, max=reach).astype(kind)


def setup_inputs(seed: int = 0, part: int = 0) -> dict:
    key_of = jax.random.split(jax.random.key(seed), 10)
    part_splits = jax.random.split(jax.random.fold_in(key_of[9], part), 10)
    draft_node_queries = draw_draft_node_queries(jax.random.fold_in(jax.random.fold_in(key_of[9], part), 71), part)
    draft_node_keys = bell_draw(part_splits[1], (TREE_NODES, KEY_VALUE_HEADS * HEAD_WIDTH), 1.0, 6.0, ((0, 4),))
    draft_node_values = bell_draw(part_splits[2], (TREE_NODES, KEY_VALUE_HEADS * HEAD_WIDTH), 1.0, 6.0, ((0, 4),))
    paged_key_cache = draw_paged_key_cache(jax.random.fold_in(jax.random.fold_in(key_of[9], part), 71), part)
    paged_value_cache = bell_draw(part_splits[4], (CACHED_LENGTH, KEY_VALUE_HEADS * HEAD_WIDTH), 1.0, 6.0, ((0, 4),))
    context_length = jax.random.randint(part_splits[5], (1,), CACHED_LENGTH // 2, CACHED_LENGTH + 1).astype(jnp.int32)
    parents = draw_parents(jax.random.fold_in(jax.random.fold_in(key_of[9], part), 71), part)
    accepted_path = draw_accepted_path(jax.random.fold_in(jax.random.fold_in(key_of[9], part), 71), part)
    out_weight = bell_draw(key_of[8], (D, QUERY_HEADS * HEAD_WIDTH), (QUERY_HEADS * HEAD_WIDTH) ** -0.5, 0.09375, ((0, 4),))
    return dict(draft_node_queries=draft_node_queries, draft_node_keys=draft_node_keys, draft_node_values=draft_node_values, paged_key_cache=paged_key_cache, paged_value_cache=paged_value_cache, context_length=context_length, parents=parents, accepted_path=accepted_path, out_weight=out_weight)


score_after_mask = -1.0e30


def ancestors(parents):
    indices = jnp.arange(TREE_NODES, dtype=jnp.int32)
    linked = (parents[:, None] == indices[None, :]) & (indices[:, None] > 0)
    ancestry = jnp.minimum(jnp.eye(TREE_NODES, dtype=jnp.float32) + linked.astype(jnp.float32), 1.0)
    for squaring in range(7):
        ancestry = jnp.minimum(jnp.dot(ancestry, ancestry, precision=lax.Precision.HIGHEST), 1.0)
    return ancestry > 0.5


def reference(draft_node_queries, draft_node_keys, draft_node_values, paged_key_cache, paged_value_cache, context_length, parents, accepted_path, out_weight):
    query_group_width = QUERY_HEADS // KEY_VALUE_HEADS
    inverse_root_scale = HEAD_WIDTH ** -0.5
    rows_per_block = min(512, CACHED_LENGTH)
    block_table = CACHED_LENGTH // rows_per_block
    length = context_length[0]
    grouped_queries = draft_node_queries.astype(jnp.float32).reshape(TREE_NODES, KEY_VALUE_HEADS, query_group_width, HEAD_WIDTH)
    gathered_key_blocks = paged_key_cache.reshape(block_table, rows_per_block, KEY_VALUE_HEADS, HEAD_WIDTH)
    gathered_value_blocks = paged_value_cache.reshape(block_table, rows_per_block, KEY_VALUE_HEADS, HEAD_WIDTH)
    starts = rows_per_block * jnp.arange(block_table, dtype=jnp.int32)
    ancestry = ancestors(parents)

    def block_scores(gathered_key_block, start_pos):
        scores = jnp.einsum("mrjz,xrz->mrjx", grouped_queries, gathered_key_block.astype(jnp.float32)) * inverse_root_scale
        usable = (start_pos + jnp.arange(rows_per_block, dtype=jnp.int32)) < length
        return jnp.where(usable, scores, score_after_mask), usable

    draft_node_scores = jnp.einsum("mrjz,xrz->mrjx", grouped_queries, draft_node_keys.astype(jnp.float32).reshape(TREE_NODES, KEY_VALUE_HEADS, HEAD_WIDTH)) * inverse_root_scale
    tree_usable = ancestry[:, None, None, :]
    draft_node_scores = jnp.where(tree_usable, draft_node_scores, score_after_mask)

    def max_step(maxima, pieces):
        scores, usable = block_scores(pieces[0], pieces[1])
        return jnp.maximum(maxima, jnp.max(scores, axis=-1)), None

    maxima, unused = lax.scan(max_step, jnp.max(draft_node_scores, axis=-1), (gathered_key_blocks, starts))

    def sum_step(state, pieces):
        totals, weighted = state
        scores, usable = block_scores(pieces[0], pieces[1])
        probs = jnp.where(usable, jnp.exp(scores - maxima[..., None]), 0.0)
        rounded = probs.astype(jnp.bfloat16).astype(jnp.float32)
        weighted = weighted + jnp.einsum("zvle,evt->zvlt", rounded, pieces[2].astype(jnp.float32))
        return (totals + jnp.sum(probs, axis=-1), weighted), None

    tree_probs = jnp.where(tree_usable, jnp.exp(draft_node_scores - maxima[..., None]), 0.0)
    draft_rounded_scores = tree_probs.astype(jnp.bfloat16).astype(jnp.float32)
    initial_weighted_sum = jnp.einsum("zvle,evt->zvlt", draft_rounded_scores, draft_node_values.astype(jnp.float32).reshape(TREE_NODES, KEY_VALUE_HEADS, HEAD_WIDTH))
    (totals, weighted), unused = lax.scan(sum_step, (jnp.sum(tree_probs, axis=-1), initial_weighted_sum), (gathered_key_blocks, starts, gathered_value_blocks))
    attention = (weighted / totals[..., None]).astype(jnp.bfloat16).reshape(TREE_NODES, QUERY_HEADS * HEAD_WIDTH)
    picker = (accepted_path[:, None] == jnp.arange(TREE_NODES, dtype=jnp.int32)[None, :]).astype(jnp.bfloat16)
    path_rows = jnp.dot(picker, attention, preferred_element_type=jnp.float32).astype(jnp.bfloat16)
    path_output = lax.dot_general(path_rows, out_weight, (((1,), (1,)), ((), ())), preferred_element_type=jnp.float32).astype(jnp.bfloat16)
    return attention, path_output
```

```python
import functools
import math

import jax
import jax.numpy as jnp
from jax import lax
from jax.experimental import pallas as pl
from jax.experimental.pallas import tpu as pltpu
from jax.sharding import PartitionSpec as P

QUERY_HEADS = 64
KEY_VALUE_HEADS = 8
HEAD_WIDTH = 64
GROUP = QUERY_HEADS // KEY_VALUE_HEADS
LANES = 128
CHUNKS = KEY_VALUE_HEADS * HEAD_WIDTH // LANES
CHUNK = 2 * GROUP * HEAD_WIDTH
PAIRS = CHUNK // LANES
EXCLUDED = -1e30
FLOOR = -1e20
SCALE = HEAD_WIDTH ** (-0.5)
NT = (((1,), (1,)), ((), ()))
MESH = pl.DeviceIdType.MESH


def kernel(
    n, own, nodes,
    length_ref, parents_ref, path_ref, q_ref, k_ref, v_ref, kc_ref, vc_ref, w_ref,
    att_ref, out_ref,
    qbuf, kbuf, vbuf, wbuf, bias, sbuf, lbuf, rbuf, rlbuf, acc,
    load_sem, q_load_sem, q_send, q_recv, p_send, p_recv, l_send, l_recv,
):
    me = lax.axis_index("blk")
    rows = q_ref.shape[0]
    wide = n * rows
    cached = kc_ref.shape[0]
    picked = path_ref.shape[0]
    peers = [lax.rem(me + k, n) for k in range(1, n)]

    q_loads = [
        pltpu.make_async_copy(
            q_ref.at[:, pl.ds(c * CHUNK, CHUNK)], qbuf.at[c, me], q_load_sem.at[c]
        )
        for c in range(CHUNKS)
    ]
    for copy in q_loads:
        copy.start()
    load_k = pltpu.make_async_copy(kc_ref, kbuf.at[pl.ds(0, cached)], load_sem.at[0])
    load_v = pltpu.make_async_copy(vc_ref, vbuf.at[pl.ds(0, cached)], load_sem.at[1])
    load_w = pltpu.make_async_copy(w_ref, wbuf, load_sem.at[2])
    load_k.start()
    load_v.start()
    load_w.start()

    barrier = pltpu.get_barrier_semaphore()
    for peer in peers:
        pl.semaphore_signal(barrier, inc=1, device_id={"blk": peer}, device_id_type=MESH)
    pl.semaphore_wait(barrier, n - 1)

    def q_copy(c, slot, peer):
        return pltpu.make_async_remote_copy(
            src_ref=qbuf.at[c, slot], dst_ref=qbuf.at[c, slot],
            send_sem=q_send.at[c, peer], recv_sem=q_recv.at[c, slot],
            device_id={"blk": peer}, device_id_type=MESH,
        )

    def p_copy(c, slot, peer):
        return pltpu.make_async_remote_copy(
            src_ref=sbuf.at[c, peer], dst_ref=rbuf.at[c, slot],
            send_sem=p_send.at[c, peer], recv_sem=p_recv.at[c, slot],
            device_id={"blk": peer}, device_id_type=MESH,
        )

    def l_copy(c, slot, peer):
        return pltpu.make_async_remote_copy(
            src_ref=lbuf.at[c, peer], dst_ref=rlbuf.at[c, slot],
            send_sem=l_send.at[c, peer], recv_sem=l_recv.at[c, slot],
            device_id={"blk": peer}, device_id_type=MESH,
        )

    for c in range(CHUNKS):
        q_loads[c].wait()
        for peer in peers:
            q_copy(c, me, peer).start()

    blank = jnp.zeros((LANES - rows, k_ref.shape[1]), jnp.float32)
    for ref, buf in ((k_ref, kbuf), (v_ref, vbuf)):
        buf[pl.ds(cached, LANES)] = jnp.concatenate(
            [ref[...].astype(jnp.float32), blank], axis=0
        ).astype(jnp.bfloat16)

    up = lax.broadcasted_iota(jnp.int32, (wide, wide), 0)
    down = lax.broadcasted_iota(jnp.int32, (wide, wide), 1)
    up_node = up // rows * own + up % rows
    links = jnp.where(up == down, 1.0, 0.0)
    for i in range(1, nodes):
        at = i // own * rows + i % own
        links = jnp.where((down == at) & (up_node == parents_ref[i]) & (up % rows < own), 1.0, links)
    for squaring in range(max(1, math.ceil(math.log2(nodes)))):
        half = links.astype(jnp.bfloat16)
        links = jnp.minimum(jnp.dot(half, half, preferred_element_type=jnp.float32), 1.0)
    source = lax.broadcasted_iota(jnp.int32, (wide, LANES), 0)
    column = lax.broadcasted_iota(jnp.int32, (wide, LANES), 1)
    mine = jnp.where((source == me * rows + column) & (column < own), 1.0, 0.0)
    related = lax.dot_general(
        links.astype(jnp.bfloat16), mine.astype(jnp.bfloat16), (((0,), (0,)), ((), ())),
        preferred_element_type=jnp.float32,
    )
    position = lax.broadcasted_iota(jnp.int32, (wide, cached), 1) + me * cached
    bias[:, pl.ds(0, cached)] = jnp.where(position < length_ref[0], 0.0, EXCLUDED)
    bias[:, pl.ds(cached, LANES)] = jnp.where(related > 0.5, 0.0, EXCLUDED)

    which = lax.broadcasted_iota(jnp.int32, (picked, wide), 0)
    spot = lax.broadcasted_iota(jnp.int32, (picked, wide), 1)
    spot_node = spot // rows * own + spot % rows
    wanted = jnp.full((picked, wide), -1, jnp.int32)
    for k in range(picked):
        wanted = jnp.where(which == k, path_ref[k], wanted)
    picker = jnp.where((wanted == spot_node) & (spot % rows < own), 1.0, 0.0)
    picker_half = picker.astype(jnp.bfloat16)

    load_k.wait()
    load_v.wait()
    lane = lax.broadcasted_iota(jnp.int32, (wide, LANES), 1)
    low = lane < HEAD_WIDTH

    def attend(c, unused):
        for peer in peers:
            q_copy(c, peer, peer).wait_recv()
        q = qbuf[c].astype(jnp.float32).reshape(wide, CHUNK)
        columns = pl.ds(pl.multiple_of(c * LANES, LANES), LANES)
        keys = kbuf[:, columns]
        values = vbuf[:, columns]
        tiles = []
        logs = jnp.full((wide, LANES), EXCLUDED, jnp.float32)
        for side in range(2):
            keep = low if side == 0 else jnp.logical_not(low)
            stacked = []
            for pair in range(PAIRS // 2):
                start = (side * PAIRS // 2 + pair) * LANES
                tile = q[:, start : start + LANES]
                turned = pltpu.roll(tile, HEAD_WIDTH, 1)
                even, odd = (tile, turned) if side == 0 else (turned, tile)
                stacked.append(jnp.where(keep, even, 0.0))
                stacked.append(jnp.where(keep, odd, 0.0))
            queries = jnp.concatenate(stacked, axis=0).astype(jnp.bfloat16)
            scores = lax.dot_general(queries, keys, NT, preferred_element_type=jnp.float32)
            scores = (
                scores.reshape(GROUP, wide, cached + LANES) + bias[...][None]
            ).reshape(GROUP * wide, cached + LANES)
            top = jnp.maximum(jnp.max(scores, axis=-1, keepdims=True), FLOOR)
            weights = jnp.exp2((scores - top) * (SCALE * math.log2(math.e)))
            total = jnp.sum(weights, axis=-1, keepdims=True)
            weighted = jnp.dot(
                weights.astype(jnp.bfloat16), values, preferred_element_type=jnp.float32
            )
            some = total > 0.0
            safe = jnp.where(some, total, 1.0)
            weighted = weighted / safe
            level = jnp.where(some, top * SCALE + jnp.log(safe), EXCLUDED)
            for head in range(GROUP):
                logs = jnp.where(
                    lane == side * GROUP + head, level[head * wide : (head + 1) * wide], logs
                )
            for pair in range(PAIRS // 2):
                even = weighted[2 * pair * wide : (2 * pair + 1) * wide]
                odd = weighted[(2 * pair + 1) * wide : (2 * pair + 2) * wide]
                if side == 0:
                    odd = pltpu.roll(odd, HEAD_WIDTH, 1)
                else:
                    even = pltpu.roll(even, HEAD_WIDTH, 1)
                tiles.append(jnp.where(low, even, odd))
        part = jnp.concatenate(tiles, axis=1)
        path_part = jnp.dot(
            picker_half, part.astype(jnp.bfloat16), preferred_element_type=jnp.float32
        )
        path_logs = jnp.dot(
            picker, logs, preferred_element_type=jnp.float32, precision=lax.Precision.HIGHEST
        )
        for d in range(n):
            mine = slice(d * rows, (d + 1) * rows)
            sbuf[c, d] = jnp.concatenate([part[mine], path_part], axis=0).astype(jnp.bfloat16)
            lbuf[c, d] = jnp.concatenate([logs[mine], path_logs], axis=0)
        for peer in peers:
            p_copy(c, me, peer).start()
            l_copy(c, me, peer).start()
        return unused

    lax.fori_loop(0, CHUNKS, attend, 0)
    load_w.wait()
    acc[...] = jnp.zeros_like(acc)
    low_out = lax.broadcasted_iota(jnp.int32, (rows + picked, LANES), 1) < HEAD_WIDTH

    def finish(c, unused):
        for peer in peers:
            p_copy(c, peer, peer).wait_recv()
            l_copy(c, peer, peer).wait_recv()
        logs = [lbuf[c, me]] + [rlbuf[c, peer] for peer in peers]
        parts = [sbuf[c, me]] + [rbuf[c, peer] for peer in peers]
        top = functools.reduce(jnp.maximum, logs)
        shares = [jnp.exp(log - top) for log in logs]
        total = functools.reduce(jnp.add, shares)
        shares = [share / total for share in shares]
        tiles = []
        for pair in range(PAIRS):
            span = slice(pair * LANES, (pair + 1) * LANES)
            tile = jnp.zeros((rows + picked, LANES), jnp.float32)
            for share, part in zip(shares, parts):
                factor = jnp.where(
                    low_out, share[:, 2 * pair : 2 * pair + 1], share[:, 2 * pair + 1 : 2 * pair + 2]
                )
                tile = tile + factor * part[:, span].astype(jnp.float32)
            tiles.append(tile)
        rows_done = jnp.concatenate(tiles, axis=1)
        columns = pl.ds(pl.multiple_of(c * CHUNK, CHUNK), CHUNK)
        att_ref[:, columns] = rows_done[:rows].astype(jnp.bfloat16)
        acc[...] += lax.dot_general(
            rows_done[rows:].astype(jnp.bfloat16), wbuf[:, columns], NT,
            preferred_element_type=jnp.float32,
        )
        return unused

    lax.fori_loop(0, CHUNKS, finish, 0)
    out_ref[...] = acc[...].astype(jnp.bfloat16)

    def drain(c, unused):
        for peer in peers:
            q_copy(c, me, peer).wait_send()
            p_copy(c, me, peer).wait_send()
            l_copy(c, me, peer).wait_send()
        return unused

    lax.fori_loop(0, CHUNKS, drain, 0)


def local(
    n,
    draft_node_queries,
    draft_node_keys,
    draft_node_values,
    paged_key_cache,
    paged_value_cache,
    context_length,
    parents,
    accepted_path,
    out_weight,
):
    own = draft_node_queries.shape[0]
    rows = -(-own // 8) * 8
    if rows != own:
        pad = ((0, rows - own), (0, 0))
        draft_node_queries = jnp.pad(draft_node_queries, pad)
        draft_node_keys = jnp.pad(draft_node_keys, pad)
        draft_node_values = jnp.pad(draft_node_values, pad)
    wide = n * rows
    cached, cache_width = paged_key_cache.shape
    picked = accepted_path.shape[0]
    smem = pl.BlockSpec(memory_space=pltpu.SMEM)
    vmem = pl.BlockSpec(memory_space=pltpu.VMEM)
    anywhere = pl.BlockSpec(memory_space=pl.ANY)
    attention, path_output = pl.pallas_call(
        functools.partial(kernel, n, own, parents.shape[0]),
        out_shape=(
            jax.ShapeDtypeStruct((rows, QUERY_HEADS * HEAD_WIDTH), jnp.bfloat16),
            jax.ShapeDtypeStruct((picked, out_weight.shape[0]), jnp.bfloat16),
        ),
        in_specs=[smem] * 3 + [anywhere, vmem, vmem] + [anywhere] * 3,
        out_specs=(vmem, vmem),
        scratch_shapes=[
            pltpu.VMEM((CHUNKS, n, rows, CHUNK), jnp.bfloat16),
            pltpu.VMEM((cached + LANES, cache_width), jnp.bfloat16),
            pltpu.VMEM((cached + LANES, cache_width), jnp.bfloat16),
            pltpu.VMEM(out_weight.shape, jnp.bfloat16),
            pltpu.VMEM((wide, cached + LANES), jnp.float32),
            pltpu.VMEM((CHUNKS, n, rows + picked, CHUNK), jnp.bfloat16),
            pltpu.VMEM((CHUNKS, n, rows + picked, LANES), jnp.float32),
            pltpu.VMEM((CHUNKS, n, rows + picked, CHUNK), jnp.bfloat16),
            pltpu.VMEM((CHUNKS, n, rows + picked, LANES), jnp.float32),
            pltpu.VMEM((picked, out_weight.shape[0]), jnp.float32),
            pltpu.SemaphoreType.DMA((3,)),
            pltpu.SemaphoreType.DMA((CHUNKS,)),
        ]
        + [pltpu.SemaphoreType.DMA((CHUNKS, n))] * 6,
        compiler_params=pltpu.CompilerParams(
            collective_id=0, has_side_effects=True, vmem_limit_bytes=56 * 1024 * 1024
        ),
        name="verify_tree",
    )(
        context_length, parents, accepted_path,
        draft_node_queries, draft_node_keys, draft_node_values,
        paged_key_cache, paged_value_cache, out_weight,
    )
    return attention[:own], path_output


def solution(mesh):
    in_specs = (
        P(("req", "blk"), None),
        P(("req", "blk"), None),
        P(("req", "blk"), None),
        P(("req", "blk"), None),
        P(("req", "blk"), None),
        P("req"),
        P("req"),
        P("req"),
        P("blk", None),
    )
    out_specs = (P(("req", "blk"), None), P("req", "blk"))
    return jax.shard_map(
        functools.partial(local, mesh.shape["blk"]),
        mesh=mesh, in_specs=in_specs, out_specs=out_specs, check_vma=False,
    )
```

```python
import functools
import math

import jax
import jax.numpy as jnp
from jax import lax
from jax.experimental import pallas as pl
from jax.experimental.pallas import tpu as pltpu
from jax.sharding import PartitionSpec as P

QUERY_HEADS = 64
KEY_VALUE_HEADS = 8
HEAD_WIDTH = 64
GROUP = QUERY_HEADS // KEY_VALUE_HEADS
LANES = 128
CHUNKS = KEY_VALUE_HEADS * HEAD_WIDTH // LANES
CHUNK = 2 * GROUP * HEAD_WIDTH
PAIRS = CHUNK // LANES
HEADS = 2 * GROUP
EXCLUDED = -1e30
FLOOR = -1e20
SCALE = HEAD_WIDTH ** (-0.5)
NT = (((1,), (1,)), ((), ()))
MESH = pl.DeviceIdType.MESH


def kernel(
    n, own, nodes,
    length_hbm, parents_hbm, path_hbm, q_ref, k_ref, v_ref, kc_ref, vc_ref, w_ref,
    att_ref, out_ref,
    length_ref, parents_ref, path_ref, kown, vown,
    qbuf, kbuf, vbuf, wbuf, bias, sbuf, rbuf, acc,
    load_sem, q_load_sem, q_send, q_recv, p_send, p_recv,
):
    me = lax.axis_index("blk")
    rows = q_ref.shape[0]
    wide = n * rows
    cached = kc_ref.shape[0]
    picked = path_hbm.shape[0]
    peers = [lax.rem(me + k, n) for k in range(1, n)]

    q_loads = [
        pltpu.make_async_copy(
            q_ref.at[:, pl.ds(c * CHUNK, CHUNK)], qbuf.at[c, me], q_load_sem.at[c]
        )
        for c in range(CHUNKS)
    ]
    for copy in q_loads:
        copy.start()
    small_loads = [
        pltpu.make_async_copy(src, dst, load_sem.at[3 + i])
        for i, (src, dst) in enumerate((
            (parents_hbm, parents_ref), (length_hbm, length_ref), (path_hbm, path_ref),
            (k_ref, kown), (v_ref, vown),
        ))
    ]
    for copy in small_loads:
        copy.start()
    load_k = pltpu.make_async_copy(kc_ref, kbuf.at[pl.ds(0, cached)], load_sem.at[0])
    load_v = pltpu.make_async_copy(vc_ref, vbuf.at[pl.ds(0, cached)], load_sem.at[1])
    load_w = pltpu.make_async_copy(w_ref, wbuf, load_sem.at[2])
    load_k.start()
    load_v.start()
    load_w.start()

    barrier = pltpu.get_barrier_semaphore()
    for peer in peers:
        pl.semaphore_signal(barrier, inc=1, device_id={"blk": peer}, device_id_type=MESH)
    pl.semaphore_wait(barrier, n - 1)

    def q_copy(c, slot, peer):
        return pltpu.make_async_remote_copy(
            src_ref=qbuf.at[c, slot], dst_ref=qbuf.at[c, slot],
            send_sem=q_send.at[c, peer], recv_sem=q_recv.at[c, slot],
            device_id={"blk": peer}, device_id_type=MESH,
        )

    def p_copy(c, slot, peer):
        return pltpu.make_async_remote_copy(
            src_ref=sbuf.at[c, peer], dst_ref=rbuf.at[c, slot],
            send_sem=p_send.at[c, peer], recv_sem=p_recv.at[c, slot],
            device_id={"blk": peer}, device_id_type=MESH,
        )

    for c in range(CHUNKS):
        q_loads[c].wait()
        for peer in peers:
            q_copy(c, me, peer).start()

    for copy in small_loads:
        copy.wait()
    blank = jnp.zeros((LANES - rows, k_ref.shape[1]), jnp.float32)
    for ref, buf in ((kown, kbuf), (vown, vbuf)):
        buf[pl.ds(cached, LANES)] = jnp.concatenate(
            [ref[...].astype(jnp.float32), blank], axis=0
        ).astype(jnp.bfloat16)

    up = lax.broadcasted_iota(jnp.int32, (wide, wide), 0)
    down = lax.broadcasted_iota(jnp.int32, (wide, wide), 1)
    up_node = up // rows * own + up % rows
    links = jnp.where(up == down, 1.0, 0.0)
    for i in range(1, nodes):
        at = i // own * rows + i % own
        links = jnp.where((down == at) & (up_node == parents_ref[i]) & (up % rows < own), 1.0, links)
    for squaring in range(max(1, math.ceil(math.log2(nodes)))):
        half = links.astype(jnp.bfloat16)
        links = jnp.minimum(jnp.dot(half, half, preferred_element_type=jnp.float32), 1.0)
    source = lax.broadcasted_iota(jnp.int32, (wide, LANES), 0)
    column = lax.broadcasted_iota(jnp.int32, (wide, LANES), 1)
    mine = jnp.where((source == me * rows + column) & (column < own), 1.0, 0.0)
    related = lax.dot_general(
        links.astype(jnp.bfloat16), mine.astype(jnp.bfloat16), (((0,), (0,)), ((), ())),
        preferred_element_type=jnp.float32,
    )
    position = lax.broadcasted_iota(jnp.int32, (wide, cached), 1) + me * cached
    bias[:, pl.ds(0, cached)] = jnp.where(position < length_ref[0], 0.0, EXCLUDED)
    bias[:, pl.ds(cached, LANES)] = jnp.where(related > 0.5, 0.0, EXCLUDED)

    which = lax.broadcasted_iota(jnp.int32, (picked, wide), 0)
    spot = lax.broadcasted_iota(jnp.int32, (picked, wide), 1)
    spot_node = spot // rows * own + spot % rows
    wanted = jnp.full((picked, wide), -1, jnp.int32)
    for k in range(picked):
        wanted = jnp.where(which == k, path_ref[k], wanted)
    picker = jnp.where((wanted == spot_node) & (spot % rows < own), 1.0, 0.0)
    picker_half = picker.astype(jnp.bfloat16)

    load_k.wait()
    load_v.wait()
    lane = lax.broadcasted_iota(jnp.int32, (wide, LANES), 1)
    low = lane < HEAD_WIDTH

    def attend(c, unused):
        for peer in peers:
            q_copy(c, peer, peer).wait_recv()
        q = qbuf[c].astype(jnp.float32).reshape(wide, CHUNK)
        columns = pl.ds(pl.multiple_of(c * LANES, LANES), LANES)
        keys = kbuf[:, columns]
        values = vbuf[:, columns]
        tiles = []
        logs = jnp.full((wide, LANES), EXCLUDED, jnp.float32)
        for side in range(2):
            keep = low if side == 0 else jnp.logical_not(low)
            stacked = []
            for pair in range(PAIRS // 2):
                start = (side * PAIRS // 2 + pair) * LANES
                tile = q[:, start : start + LANES]
                turned = pltpu.roll(tile, HEAD_WIDTH, 1)
                even, odd = (tile, turned) if side == 0 else (turned, tile)
                stacked.append(jnp.where(keep, even, 0.0))
                stacked.append(jnp.where(keep, odd, 0.0))
            queries = jnp.concatenate(stacked, axis=0).astype(jnp.bfloat16)
            scores = lax.dot_general(queries, keys, NT, preferred_element_type=jnp.float32)
            scores = (
                scores.reshape(GROUP, wide, cached + LANES) + bias[...][None]
            ).reshape(GROUP * wide, cached + LANES)
            top = jnp.maximum(jnp.max(scores, axis=-1, keepdims=True), FLOOR)
            weights = jnp.exp2((scores - top) * (SCALE * math.log2(math.e)))
            total = jnp.sum(weights, axis=-1, keepdims=True)
            weighted = jnp.dot(
                weights.astype(jnp.bfloat16), values, preferred_element_type=jnp.float32
            )
            some = total > 0.0
            safe = jnp.where(some, total, 1.0)
            weighted = weighted / safe
            level = jnp.where(some, top * SCALE + jnp.log(safe), EXCLUDED)
            for head in range(GROUP):
                logs = jnp.where(
                    lane == side * GROUP + head, level[head * wide : (head + 1) * wide], logs
                )
            for pair in range(PAIRS // 2):
                even = weighted[2 * pair * wide : (2 * pair + 1) * wide]
                odd = weighted[(2 * pair + 1) * wide : (2 * pair + 2) * wide]
                if side == 0:
                    odd = pltpu.roll(odd, HEAD_WIDTH, 1)
                else:
                    even = pltpu.roll(even, HEAD_WIDTH, 1)
                tiles.append(jnp.where(low, even, odd))
        first = logs.astype(jnp.bfloat16).astype(jnp.float32)
        rest = logs - first
        second = rest.astype(jnp.bfloat16).astype(jnp.float32)
        third = rest - second
        tiles.append(
            jnp.where(
                lane < HEADS, first,
                jnp.where(
                    lane < 2 * HEADS, pltpu.roll(second, HEADS, 1),
                    jnp.where(lane < 3 * HEADS, pltpu.roll(third, 2 * HEADS, 1), 0.0),
                ),
            )
        )
        part = jnp.concatenate(tiles, axis=1)
        path_part = jnp.dot(
            picker_half, part.astype(jnp.bfloat16), preferred_element_type=jnp.float32
        )
        for d in range(n):
            mine = slice(d * rows, (d + 1) * rows)
            sbuf[c, d] = jnp.concatenate([part[mine], path_part], axis=0).astype(jnp.bfloat16)
        for peer in peers:
            p_copy(c, me, peer).start()
        return unused

    lax.fori_loop(0, CHUNKS, attend, 0)
    load_w.wait()
    acc[...] = jnp.zeros_like(acc)
    low_out = lax.broadcasted_iota(jnp.int32, (rows + picked, LANES), 1) < HEAD_WIDTH

    def finish(c, unused):
        for peer in peers:
            p_copy(c, peer, peer).wait_recv()
        parts = [sbuf[c, me]] + [rbuf[c, peer] for peer in peers]
        logs = []
        for part in parts:
            terms = part[:, CHUNK:].astype(jnp.float32)
            logs.append(
                terms
                + pltpu.roll(terms, LANES - HEADS, 1)
                + pltpu.roll(terms, LANES - 2 * HEADS, 1)
            )
        top = functools.reduce(jnp.maximum, logs)
        shares = [jnp.exp(log - top) for log in logs]
        total = functools.reduce(jnp.add, shares)
        shares = [share / total for share in shares]
        tiles = []
        for pair in range(PAIRS):
            span = slice(pair * LANES, (pair + 1) * LANES)
            tile = jnp.zeros((rows + picked, LANES), jnp.float32)
            for share, part in zip(shares, parts):
                factor = jnp.where(
                    low_out, share[:, 2 * pair : 2 * pair + 1], share[:, 2 * pair + 1 : 2 * pair + 2]
                )
                tile = tile + factor * part[:, span].astype(jnp.float32)
            tiles.append(tile)
        rows_done = jnp.concatenate(tiles, axis=1)
        columns = pl.ds(pl.multiple_of(c * CHUNK, CHUNK), CHUNK)
        att_ref[:, columns] = rows_done[:rows].astype(jnp.bfloat16)
        acc[...] += lax.dot_general(
            rows_done[rows:].astype(jnp.bfloat16), wbuf[:, columns], NT,
            preferred_element_type=jnp.float32,
        )
        return unused

    lax.fori_loop(0, CHUNKS, finish, 0)
    out_ref[...] = acc[...].astype(jnp.bfloat16)

    def drain(c, unused):
        for peer in peers:
            q_copy(c, me, peer).wait_send()
            p_copy(c, me, peer).wait_send()
        return unused

    lax.fori_loop(0, CHUNKS, drain, 0)


def write_out(att_ref, out_ref, att_hbm, out_hbm, sems):
    copies = [
        pltpu.make_async_copy(att_ref, att_hbm, sems.at[0]),
        pltpu.make_async_copy(out_ref, out_hbm, sems.at[1]),
    ]
    for copy in copies:
        copy.start()
    for copy in copies:
        copy.wait()


def local(
    n,
    draft_node_queries,
    draft_node_keys,
    draft_node_values,
    paged_key_cache,
    paged_value_cache,
    context_length,
    parents,
    accepted_path,
    out_weight,
):
    own = draft_node_queries.shape[0]
    rows = -(-own // 8) * 8
    if rows != own:
        pad = ((0, rows - own), (0, 0))
        draft_node_queries = jnp.pad(draft_node_queries, pad)
        draft_node_keys = jnp.pad(draft_node_keys, pad)
        draft_node_values = jnp.pad(draft_node_values, pad)
    wide = n * rows
    cached, cache_width = paged_key_cache.shape
    picked = accepted_path.shape[0]
    vmem = pl.BlockSpec(memory_space=pltpu.VMEM)
    anywhere = pl.BlockSpec(memory_space=pltpu.HBM)
    shapes = (
        jax.ShapeDtypeStruct((rows, QUERY_HEADS * HEAD_WIDTH), jnp.bfloat16),
        jax.ShapeDtypeStruct((picked, out_weight.shape[0]), jnp.bfloat16),
    )
    held = pl.pallas_call(
        functools.partial(kernel, n, own, parents.shape[0]),
        out_shape=tuple(pltpu.VMEM(shape.shape, shape.dtype) for shape in shapes),
        in_specs=[anywhere] * 9,
        out_specs=(vmem, vmem),
        scratch_shapes=[
            pltpu.SMEM(context_length.shape, jnp.int32),
            pltpu.SMEM(parents.shape, jnp.int32),
            pltpu.SMEM(accepted_path.shape, jnp.int32),
            pltpu.VMEM((rows, cache_width), jnp.bfloat16),
            pltpu.VMEM((rows, cache_width), jnp.bfloat16),
            pltpu.VMEM((CHUNKS, n, rows, CHUNK), jnp.bfloat16),
            pltpu.VMEM((cached + LANES, cache_width), jnp.bfloat16),
            pltpu.VMEM((cached + LANES, cache_width), jnp.bfloat16),
            pltpu.VMEM(out_weight.shape, jnp.bfloat16),
            pltpu.VMEM((wide, cached + LANES), jnp.float32),
            pltpu.VMEM((CHUNKS, n, rows + picked, CHUNK + LANES), jnp.bfloat16),
            pltpu.VMEM((CHUNKS, n, rows + picked, CHUNK + LANES), jnp.bfloat16),
            pltpu.VMEM((picked, out_weight.shape[0]), jnp.float32),
            pltpu.SemaphoreType.DMA((8,)),
            pltpu.SemaphoreType.DMA((CHUNKS,)),
        ]
        + [pltpu.SemaphoreType.DMA((CHUNKS, n))] * 4,
        compiler_params=pltpu.CompilerParams(
            collective_id=0, has_side_effects=True, vmem_limit_bytes=56 * 1024 * 1024
        ),
        name="verify_tree",
    )(
        context_length, parents, accepted_path,
        draft_node_queries, draft_node_keys, draft_node_values,
        paged_key_cache, paged_value_cache, out_weight,
    )
    attention, path_output = pl.pallas_call(
        write_out,
        out_shape=shapes,
        in_specs=(vmem, vmem),
        out_specs=(anywhere, anywhere),
        scratch_shapes=[pltpu.SemaphoreType.DMA((2,))],
        compiler_params=pltpu.CompilerParams(vmem_limit_bytes=1024 * 1024),
        name="write_out",
    )(*held)
    return attention[:own], path_output


def solution(mesh):
    in_specs = (
        P(("req", "blk"), None),
        P(("req", "blk"), None),
        P(("req", "blk"), None),
        P(("req", "blk"), None),
        P(("req", "blk"), None),
        P("req"),
        P("req"),
        P("req"),
        P("blk", None),
    )
    out_specs = (P(("req", "blk"), None), P("req", "blk"))
    return jax.shard_map(
        functools.partial(local, mesh.shape["blk"]),
        mesh=mesh, in_specs=in_specs, out_specs=out_specs, check_vma=False,
    )
```

```python
import functools
import math

import jax
import jax.numpy as jnp
from jax import lax
from jax.experimental import pallas as pl
from jax.experimental.pallas import tpu as pltpu
from jax.sharding import PartitionSpec as P

QUERY_HEADS = 64
KEY_VALUE_HEADS = 8
HEAD_WIDTH = 64
GROUP = QUERY_HEADS // KEY_VALUE_HEADS
LANES = 128
CHUNKS = KEY_VALUE_HEADS * HEAD_WIDTH // LANES
CHUNK = 2 * GROUP * HEAD_WIDTH
PAIRS = CHUNK // LANES
HEADS = 2 * GROUP
EXCLUDED = -1e30
FLOOR = -1e20
SCALE = HEAD_WIDTH ** (-0.5)
NT = (((1,), (1,)), ((), ()))
MESH = pl.DeviceIdType.MESH


def partner(me, k, n):
    if n & (n - 1):
        return lax.rem(me + k, n)
    other = me
    bit = 1
    while bit < n:
        if k & bit:
            other = other + bit - 2 * bit * ((me // bit) % 2)
        bit *= 2
    return other


def kernel(
    n, own, nodes,
    length_hbm, parents_hbm, path_hbm, q_ref, k_ref, v_ref, kc_ref, vc_ref, w_ref,
    att_ref, out_ref,
    length_ref, parents_ref, path_ref, kown, vown,
    qbuf, kbuf, vbuf, wbuf, bias, sbuf, rbuf, acc,
    load_sem, q_load_sem, q_send, q_recv, p_send, p_recv,
):
    me = lax.axis_index("blk")
    rows = q_ref.shape[0]
    wide = n * rows
    cached = kc_ref.shape[0]
    picked = path_hbm.shape[0]
    peers = [partner(me, k, n) for k in range(n - 1, 0, -1)]

    q_loads = [
        pltpu.make_async_copy(
            q_ref.at[:, pl.ds(c * CHUNK, CHUNK)], qbuf.at[c, me], q_load_sem.at[c]
        )
        for c in range(CHUNKS)
    ]
    for copy in q_loads:
        copy.start()
    load_k = pltpu.make_async_copy(kc_ref, kbuf.at[pl.ds(0, cached)], load_sem.at[0])
    load_v = pltpu.make_async_copy(vc_ref, vbuf.at[pl.ds(0, cached)], load_sem.at[1])
    load_w = pltpu.make_async_copy(w_ref, wbuf, load_sem.at[2])

    small_loads = [
        pltpu.make_async_copy(src, dst, load_sem.at[3 + i])
        for i, (src, dst) in enumerate((
            (parents_hbm, parents_ref), (length_hbm, length_ref), (path_hbm, path_ref),
            (k_ref, kown), (v_ref, vown),
        ))
    ]
    for copy in small_loads:
        copy.start()

    barrier = pltpu.get_barrier_semaphore()
    for peer in peers:
        pl.semaphore_signal(barrier, inc=1, device_id={"blk": peer}, device_id_type=MESH)
    pl.semaphore_wait(barrier, n - 1)

    def q_copy(c, slot, peer):
        return pltpu.make_async_remote_copy(
            src_ref=qbuf.at[c, slot], dst_ref=qbuf.at[c, slot],
            send_sem=q_send.at[c, peer], recv_sem=q_recv.at[c, slot],
            device_id={"blk": peer}, device_id_type=MESH,
        )

    def p_copy(c, slot, peer):
        return pltpu.make_async_remote_copy(
            src_ref=sbuf.at[c, peer], dst_ref=rbuf.at[c, slot],
            send_sem=p_send.at[c, peer], recv_sem=p_recv.at[c, slot],
            device_id={"blk": peer}, device_id_type=MESH,
        )

    for c in range(CHUNKS):
        q_loads[c].wait()
        for peer in peers:
            q_copy(c, me, peer).start()
    load_k.start()
    load_v.start()
    load_w.start()

    for copy in small_loads:
        copy.wait()
    blank = jnp.zeros((LANES - rows, k_ref.shape[1]), jnp.float32)
    for ref, buf in ((kown, kbuf), (vown, vbuf)):
        buf[pl.ds(cached, LANES)] = jnp.concatenate(
            [ref[...].astype(jnp.float32), blank], axis=0
        ).astype(jnp.bfloat16)

    up = lax.broadcasted_iota(jnp.int32, (wide, wide), 0)
    down = lax.broadcasted_iota(jnp.int32, (wide, wide), 1)
    up_node = up // rows * own + up % rows
    links = jnp.where(up == down, 1.0, 0.0)
    for i in range(1, nodes):
        at = i // own * rows + i % own
        links = jnp.where((down == at) & (up_node == parents_ref[i]) & (up % rows < own), 1.0, links)
    for squaring in range(max(1, math.ceil(math.log2(nodes)))):
        half = links.astype(jnp.bfloat16)
        links = jnp.minimum(jnp.dot(half, half, preferred_element_type=jnp.float32), 1.0)
    source = lax.broadcasted_iota(jnp.int32, (wide, LANES), 0)
    column = lax.broadcasted_iota(jnp.int32, (wide, LANES), 1)
    mine = jnp.where((source == me * rows + column) & (column < own), 1.0, 0.0)
    related = lax.dot_general(
        links.astype(jnp.bfloat16), mine.astype(jnp.bfloat16), (((0,), (0,)), ((), ())),
        preferred_element_type=jnp.float32,
    )
    position = lax.broadcasted_iota(jnp.int32, (wide, cached), 1) + me * cached
    bias[:, pl.ds(0, cached)] = jnp.where(position < length_ref[0], 0.0, EXCLUDED)
    bias[:, pl.ds(cached, LANES)] = jnp.where(related > 0.5, 0.0, EXCLUDED)

    which = lax.broadcasted_iota(jnp.int32, (picked, wide), 0)
    spot = lax.broadcasted_iota(jnp.int32, (picked, wide), 1)
    spot_node = spot // rows * own + spot % rows
    wanted = jnp.full((picked, wide), -1, jnp.int32)
    for k in range(picked):
        wanted = jnp.where(which == k, path_ref[k], wanted)
    picker = jnp.where((wanted == spot_node) & (spot % rows < own), 1.0, 0.0)
    picker_half = picker.astype(jnp.bfloat16)

    load_k.wait()
    load_v.wait()
    lane = lax.broadcasted_iota(jnp.int32, (wide, LANES), 1)
    low = lane < HEAD_WIDTH

    def attend(c, unused):
        for peer in peers:
            q_copy(c, peer, peer).wait_recv()
        q = qbuf[c].astype(jnp.float32).reshape(wide, CHUNK)
        columns = pl.ds(pl.multiple_of(c * LANES, LANES), LANES)
        keys = kbuf[:, columns]
        values = vbuf[:, columns]
        tiles = []
        logs = jnp.full((wide, LANES), EXCLUDED, jnp.float32)
        for side in range(2):
            keep = low if side == 0 else jnp.logical_not(low)
            stacked = []
            for pair in range(PAIRS // 2):
                start = (side * PAIRS // 2 + pair) * LANES
                tile = q[:, start : start + LANES]
                turned = pltpu.roll(tile, HEAD_WIDTH, 1)
                even, odd = (tile, turned) if side == 0 else (turned, tile)
                stacked.append(jnp.where(keep, even, 0.0))
                stacked.append(jnp.where(keep, odd, 0.0))
            queries = jnp.concatenate(stacked, axis=0).astype(jnp.bfloat16)
            scores = lax.dot_general(queries, keys, NT, preferred_element_type=jnp.float32)
            scores = (
                scores.reshape(GROUP, wide, cached + LANES) + bias[...][None]
            ).reshape(GROUP * wide, cached + LANES)
            top = jnp.maximum(jnp.max(scores, axis=-1, keepdims=True), FLOOR)
            weights = jnp.exp2((scores - top) * (SCALE * math.log2(math.e)))
            total = jnp.sum(weights, axis=-1, keepdims=True)
            weighted = jnp.dot(
                weights.astype(jnp.bfloat16), values, preferred_element_type=jnp.float32
            )
            some = total > 0.0
            safe = jnp.where(some, total, 1.0)
            weighted = weighted / safe
            level = jnp.where(some, top * SCALE + jnp.log(safe), EXCLUDED)
            for head in range(GROUP):
                logs = jnp.where(
                    lane == side * GROUP + head, level[head * wide : (head + 1) * wide], logs
                )
            for pair in range(PAIRS // 2):
                even = weighted[2 * pair * wide : (2 * pair + 1) * wide]
                odd = weighted[(2 * pair + 1) * wide : (2 * pair + 2) * wide]
                if side == 0:
                    odd = pltpu.roll(odd, HEAD_WIDTH, 1)
                else:
                    even = pltpu.roll(even, HEAD_WIDTH, 1)
                tiles.append(jnp.where(low, even, odd))
        first = logs.astype(jnp.bfloat16).astype(jnp.float32)
        rest = logs - first
        second = rest.astype(jnp.bfloat16).astype(jnp.float32)
        third = rest - second
        tiles.append(
            jnp.where(
                lane < HEADS, first,
                jnp.where(
                    lane < 2 * HEADS, pltpu.roll(second, HEADS, 1),
                    jnp.where(lane < 3 * HEADS, pltpu.roll(third, 2 * HEADS, 1), 0.0),
                ),
            )
        )
        part = jnp.concatenate(tiles, axis=1)
        path_part = jnp.dot(
            picker_half, part.astype(jnp.bfloat16), preferred_element_type=jnp.float32
        )
        for d in range(n):
            mine = slice(d * rows, (d + 1) * rows)
            sbuf[c, d] = jnp.concatenate([part[mine], path_part], axis=0).astype(jnp.bfloat16)
        for peer in peers:
            p_copy(c, me, peer).start()
        return unused

    lax.fori_loop(0, CHUNKS, attend, 0)
    load_w.wait()
    acc[...] = jnp.zeros_like(acc)
    low_out = lax.broadcasted_iota(jnp.int32, (rows + picked, LANES), 1) < HEAD_WIDTH

    def finish(c, unused):
        for peer in peers:
            p_copy(c, peer, peer).wait_recv()
        parts = [sbuf[c, me]] + [rbuf[c, peer] for peer in peers]
        logs = []
        for part in parts:
            terms = part[:, CHUNK:].astype(jnp.float32)
            logs.append(
                terms
                + pltpu.roll(terms, LANES - HEADS, 1)
                + pltpu.roll(terms, LANES - 2 * HEADS, 1)
            )
        top = functools.reduce(jnp.maximum, logs)
        shares = [jnp.exp(log - top) for log in logs]
        total = functools.reduce(jnp.add, shares)
        shares = [share / total for share in shares]
        tiles = []
        for pair in range(PAIRS):
            span = slice(pair * LANES, (pair + 1) * LANES)
            tile = jnp.zeros((rows + picked, LANES), jnp.float32)
            for share, part in zip(shares, parts):
                factor = jnp.where(
                    low_out, share[:, 2 * pair : 2 * pair + 1], share[:, 2 * pair + 1 : 2 * pair + 2]
                )
                tile = tile + factor * part[:, span].astype(jnp.float32)
            tiles.append(tile)
        rows_done = jnp.concatenate(tiles, axis=1)
        columns = pl.ds(pl.multiple_of(c * CHUNK, CHUNK), CHUNK)
        att_ref[:, columns] = rows_done[:rows].astype(jnp.bfloat16)
        acc[...] += lax.dot_general(
            rows_done[rows:].astype(jnp.bfloat16), wbuf[:, columns], NT,
            preferred_element_type=jnp.float32,
        )
        return unused

    lax.fori_loop(0, CHUNKS, finish, 0)
    out_ref[...] = acc[...].astype(jnp.bfloat16)

    def drain(c, unused):
        for peer in peers:
            q_copy(c, me, peer).wait_send()
            p_copy(c, me, peer).wait_send()
        return unused

    lax.fori_loop(0, CHUNKS, drain, 0)


def write_out(att_ref, out_ref, att_hbm, out_hbm, sems):
    copies = [
        pltpu.make_async_copy(att_ref, att_hbm, sems.at[0]),
        pltpu.make_async_copy(out_ref, out_hbm, sems.at[1]),
    ]
    for copy in copies:
        copy.start()
    for copy in copies:
        copy.wait()


def local(
    n,
    draft_node_queries,
    draft_node_keys,
    draft_node_values,
    paged_key_cache,
    paged_value_cache,
    context_length,
    parents,
    accepted_path,
    out_weight,
):
    own = draft_node_queries.shape[0]
    rows = -(-own // 8) * 8
    if rows != own:
        pad = ((0, rows - own), (0, 0))
        draft_node_queries = jnp.pad(draft_node_queries, pad)
        draft_node_keys = jnp.pad(draft_node_keys, pad)
        draft_node_values = jnp.pad(draft_node_values, pad)
    wide = n * rows
    cached, cache_width = paged_key_cache.shape
    picked = accepted_path.shape[0]
    vmem = pl.BlockSpec(memory_space=pltpu.VMEM)
    anywhere = pl.BlockSpec(memory_space=pltpu.HBM)
    shapes = (
        jax.ShapeDtypeStruct((rows, QUERY_HEADS * HEAD_WIDTH), jnp.bfloat16),
        jax.ShapeDtypeStruct((picked, out_weight.shape[0]), jnp.bfloat16),
    )
    held = pl.pallas_call(
        functools.partial(kernel, n, own, parents.shape[0]),
        out_shape=tuple(pltpu.VMEM(shape.shape, shape.dtype) for shape in shapes),
        in_specs=[anywhere] * 9,
        out_specs=(vmem, vmem),
        scratch_shapes=[
            pltpu.SMEM(context_length.shape, jnp.int32),
            pltpu.SMEM(parents.shape, jnp.int32),
            pltpu.SMEM(accepted_path.shape, jnp.int32),
            pltpu.VMEM((rows, cache_width), jnp.bfloat16),
            pltpu.VMEM((rows, cache_width), jnp.bfloat16),
            pltpu.VMEM((CHUNKS, n, rows, CHUNK), jnp.bfloat16),
            pltpu.VMEM((cached + LANES, cache_width), jnp.bfloat16),
            pltpu.VMEM((cached + LANES, cache_width), jnp.bfloat16),
            pltpu.VMEM(out_weight.shape, jnp.bfloat16),
            pltpu.VMEM((wide, cached + LANES), jnp.float32),
            pltpu.VMEM((CHUNKS, n, rows + picked, CHUNK + LANES), jnp.bfloat16),
            pltpu.VMEM((CHUNKS, n, rows + picked, CHUNK + LANES), jnp.bfloat16),
            pltpu.VMEM((picked, out_weight.shape[0]), jnp.float32),
            pltpu.SemaphoreType.DMA((8,)),
            pltpu.SemaphoreType.DMA((CHUNKS,)),
        ]
        + [pltpu.SemaphoreType.DMA((CHUNKS, n))] * 4,
        compiler_params=pltpu.CompilerParams(
            collective_id=0, has_side_effects=True, vmem_limit_bytes=56 * 1024 * 1024
        ),
        name="verify_tree",
    )(
        context_length, parents, accepted_path,
        draft_node_queries, draft_node_keys, draft_node_values,
        paged_key_cache, paged_value_cache, out_weight,
    )
    attention, path_output = pl.pallas_call(
        write_out,
        out_shape=shapes,
        in_specs=(vmem, vmem),
        out_specs=(anywhere, anywhere),
        scratch_shapes=[pltpu.SemaphoreType.DMA((2,))],
        compiler_params=pltpu.CompilerParams(vmem_limit_bytes=1024 * 1024),
        name="write_out",
    )(*held)
    return attention[:own], path_output


def solution(mesh):
    in_specs = (
        P(("req", "blk"), None),
        P(("req", "blk"), None),
        P(("req", "blk"), None),
        P(("req", "blk"), None),
        P(("req", "blk"), None),
        P("req"),
        P("req"),
        P("req"),
        P("blk", None),
    )
    out_specs = (P(("req", "blk"), None), P("req", "blk"))
    return jax.shard_map(
        functools.partial(local, mesh.shape["blk"]),
        mesh=mesh, in_specs=in_specs, out_specs=out_specs, check_vma=False,
    )
```

```python
import functools
import math

import jax
import jax.numpy as jnp
from jax import lax
from jax.experimental import pallas as pl
from jax.experimental.pallas import tpu as pltpu
from jax.sharding import PartitionSpec as P

QUERY_HEADS = 64
KEY_VALUE_HEADS = 8
HEAD_WIDTH = 64
GROUP = QUERY_HEADS // KEY_VALUE_HEADS
LANES = 128
CHUNKS = KEY_VALUE_HEADS * HEAD_WIDTH // LANES
CHUNK = 2 * GROUP * HEAD_WIDTH
PAIRS = CHUNK // LANES
HEADS = 2 * GROUP
EXCLUDED = -1e30
FLOOR = -1e20
SCALE = HEAD_WIDTH ** (-0.5)
NT = (((1,), (1,)), ((), ()))
MESH = pl.DeviceIdType.MESH


def partner(me, k, n):
    if n & (n - 1):
        return lax.rem(me + k, n)
    other = me
    bit = 1
    while bit < n:
        if k & bit:
            other = other + bit - 2 * bit * ((me // bit) % 2)
        bit *= 2
    return other


def kernel(
    n, own, nodes,
    length_hbm, parents_hbm, path_hbm, q_ref, k_ref, v_ref, kc_ref, vc_ref, w_ref,
    att_ref, out_ref,
    length_ref, parents_ref, path_ref, kown, vown,
    qbuf, kbuf, vbuf, wbuf, bias, sbuf, rbuf, acc,
    load_sem, q_load_sem, q_send, q_recv, p_send, p_recv,
):
    me = lax.axis_index("blk")
    rows = q_ref.shape[0]
    wide = n * rows
    cached = kc_ref.shape[0]
    picked = path_hbm.shape[0]
    peers = [partner(me, k, n) for k in range(n - 1, 0, -1)]

    q_loads = [
        pltpu.make_async_copy(
            q_ref.at[:, pl.ds(c * CHUNK, CHUNK)], qbuf.at[c, me], q_load_sem.at[c]
        )
        for c in range(CHUNKS)
    ]
    for copy in q_loads:
        copy.start()
    load_k = pltpu.make_async_copy(kc_ref, kbuf.at[pl.ds(0, cached)], load_sem.at[0])
    load_v = pltpu.make_async_copy(vc_ref, vbuf.at[pl.ds(0, cached)], load_sem.at[1])
    load_w = pltpu.make_async_copy(w_ref, wbuf, load_sem.at[2])

    small_loads = [
        pltpu.make_async_copy(src, dst, load_sem.at[3 + i])
        for i, (src, dst) in enumerate((
            (parents_hbm, parents_ref), (length_hbm, length_ref), (path_hbm, path_ref),
            (k_ref, kown), (v_ref, vown),
        ))
    ]
    for copy in small_loads:
        copy.start()

    barrier = pltpu.get_barrier_semaphore()
    for peer in peers:
        pl.semaphore_signal(barrier, inc=1, device_id={"blk": peer}, device_id_type=MESH)
    pl.semaphore_wait(barrier, n - 1)

    def q_copy(c, slot, peer):
        return pltpu.make_async_remote_copy(
            src_ref=qbuf.at[c, slot], dst_ref=qbuf.at[c, slot],
            send_sem=q_send.at[c, peer], recv_sem=q_recv.at[c, slot],
            device_id={"blk": peer}, device_id_type=MESH,
        )

    def p_copy(c, slot, peer):
        return pltpu.make_async_remote_copy(
            src_ref=sbuf.at[c, peer], dst_ref=rbuf.at[c, slot],
            send_sem=p_send.at[c, peer], recv_sem=p_recv.at[c, slot],
            device_id={"blk": peer}, device_id_type=MESH,
        )

    for c in range(CHUNKS):
        q_loads[c].wait()
        for peer in peers:
            q_copy(c, me, peer).start()
    load_k.start()
    load_v.start()
    load_w.start()

    for copy in small_loads:
        copy.wait()
    blank = jnp.zeros((LANES - rows, k_ref.shape[1]), jnp.float32)
    for ref, buf in ((kown, kbuf), (vown, vbuf)):
        buf[pl.ds(cached, LANES)] = jnp.concatenate(
            [ref[...].astype(jnp.float32), blank], axis=0
        ).astype(jnp.bfloat16)

    up = lax.broadcasted_iota(jnp.int32, (wide, wide), 0)
    down = lax.broadcasted_iota(jnp.int32, (wide, wide), 1)
    up_node = up // rows * own + up % rows
    links = jnp.where(up == down, 1.0, 0.0)
    for i in range(1, nodes):
        at = i // own * rows + i % own
        links = jnp.where((down == at) & (up_node == parents_ref[i]) & (up % rows < own), 1.0, links)
    for squaring in range(max(1, math.ceil(math.log2(nodes)))):
        half = links.astype(jnp.bfloat16)
        links = jnp.minimum(jnp.dot(half, half, preferred_element_type=jnp.float32), 1.0)
    source = lax.broadcasted_iota(jnp.int32, (wide, LANES), 0)
    column = lax.broadcasted_iota(jnp.int32, (wide, LANES), 1)
    mine = jnp.where((source == me * rows + column) & (column < own), 1.0, 0.0)
    related = lax.dot_general(
        links.astype(jnp.bfloat16), mine.astype(jnp.bfloat16), (((0,), (0,)), ((), ())),
        preferred_element_type=jnp.float32,
    )
    position = lax.broadcasted_iota(jnp.int32, (wide, cached), 1) + me * cached
    bias[:, pl.ds(0, cached)] = jnp.where(position < length_ref[0], 0.0, EXCLUDED)
    bias[:, pl.ds(cached, LANES)] = jnp.where(related > 0.5, 0.0, EXCLUDED)

    which = lax.broadcasted_iota(jnp.int32, (picked, wide), 0)
    spot = lax.broadcasted_iota(jnp.int32, (picked, wide), 1)
    spot_node = spot // rows * own + spot % rows
    wanted = jnp.full((picked, wide), -1, jnp.int32)
    for k in range(picked):
        wanted = jnp.where(which == k, path_ref[k], wanted)
    picker = jnp.where((wanted == spot_node) & (spot % rows < own), 1.0, 0.0)
    picker_half = picker.astype(jnp.bfloat16)

    load_k.wait()
    load_v.wait()
    lane = lax.broadcasted_iota(jnp.int32, (wide, LANES), 1)
    low = lane < HEAD_WIDTH

    def attend(c, unused):
        for peer in peers:
            q_copy(c, peer, peer).wait_recv()
        q = qbuf[c].astype(jnp.float32).reshape(wide, CHUNK)
        columns = pl.ds(pl.multiple_of(c * LANES, LANES), LANES)
        keys = kbuf[:, columns]
        values = vbuf[:, columns]
        tiles = []
        logs = jnp.full((wide, LANES), EXCLUDED, jnp.float32)
        for side in range(2):
            keep = low if side == 0 else jnp.logical_not(low)
            stacked = []
            for pair in range(PAIRS // 2):
                start = (side * PAIRS // 2 + pair) * LANES
                tile = q[:, start : start + LANES]
                turned = pltpu.roll(tile, HEAD_WIDTH, 1)
                even, odd = (tile, turned) if side == 0 else (turned, tile)
                stacked.append(jnp.where(keep, even, 0.0))
                stacked.append(jnp.where(keep, odd, 0.0))
            queries = jnp.concatenate(stacked, axis=0).astype(jnp.bfloat16)
            scores = lax.dot_general(queries, keys, NT, preferred_element_type=jnp.float32)
            scores = (
                scores.reshape(GROUP, wide, cached + LANES) + bias[...][None]
            ).reshape(GROUP * wide, cached + LANES)
            top = jnp.maximum(jnp.max(scores, axis=-1, keepdims=True), FLOOR)
            weights = jnp.exp2((scores - top) * (SCALE * math.log2(math.e)))
            total = jnp.sum(weights, axis=-1, keepdims=True)
            weighted = jnp.dot(
                weights.astype(jnp.bfloat16), values, preferred_element_type=jnp.float32
            )
            some = total > 0.0
            safe = jnp.where(some, total, 1.0)
            weighted = weighted / safe
            level = jnp.where(some, top * SCALE + jnp.log(safe), EXCLUDED)
            for head in range(GROUP):
                logs = jnp.where(
                    lane == side * GROUP + head, level[head * wide : (head + 1) * wide], logs
                )
            for pair in range(PAIRS // 2):
                even = weighted[2 * pair * wide : (2 * pair + 1) * wide]
                odd = weighted[(2 * pair + 1) * wide : (2 * pair + 2) * wide]
                if side == 0:
                    odd = pltpu.roll(odd, HEAD_WIDTH, 1)
                else:
                    even = pltpu.roll(even, HEAD_WIDTH, 1)
                tiles.append(jnp.where(low, even, odd))
        first = logs.astype(jnp.bfloat16).astype(jnp.float32)
        rest = logs - first
        second = rest.astype(jnp.bfloat16).astype(jnp.float32)
        third = rest - second
        tiles.append(
            jnp.where(
                lane < HEADS, first,
                jnp.where(
                    lane < 2 * HEADS, pltpu.roll(second, HEADS, 1),
                    jnp.where(lane < 3 * HEADS, pltpu.roll(third, 2 * HEADS, 1), 0.0),
                ),
            )
        )
        part = jnp.concatenate(tiles, axis=1)
        path_part = jnp.dot(
            picker_half, part.astype(jnp.bfloat16), preferred_element_type=jnp.float32
        )
        for d in range(n):
            mine = slice(d * rows, (d + 1) * rows)
            sbuf[c, d] = jnp.concatenate([part[mine], path_part], axis=0).astype(jnp.bfloat16)
        for peer in peers:
            p_copy(c, me, peer).start()
        return unused

    lax.fori_loop(0, CHUNKS, attend, 0, unroll=True)
    load_w.wait()
    acc[...] = jnp.zeros_like(acc)
    low_out = lax.broadcasted_iota(jnp.int32, (rows + picked, LANES), 1) < HEAD_WIDTH

    def finish(c, unused):
        for peer in peers:
            p_copy(c, peer, peer).wait_recv()
        parts = [sbuf[c, me]] + [rbuf[c, peer] for peer in peers]
        logs = []
        for part in parts:
            terms = part[:, CHUNK:].astype(jnp.float32)
            logs.append(
                terms
                + pltpu.roll(terms, LANES - HEADS, 1)
                + pltpu.roll(terms, LANES - 2 * HEADS, 1)
            )
        top = functools.reduce(jnp.maximum, logs)
        shares = [jnp.exp(log - top) for log in logs]
        total = functools.reduce(jnp.add, shares)
        shares = [share / total for share in shares]
        tiles = []
        for pair in range(PAIRS):
            span = slice(pair * LANES, (pair + 1) * LANES)
            tile = jnp.zeros((rows + picked, LANES), jnp.float32)
            for share, part in zip(shares, parts):
                factor = jnp.where(
                    low_out, share[:, 2 * pair : 2 * pair + 1], share[:, 2 * pair + 1 : 2 * pair + 2]
                )
                tile = tile + factor * part[:, span].astype(jnp.float32)
            tiles.append(tile)
        rows_done = jnp.concatenate(tiles, axis=1)
        columns = pl.ds(pl.multiple_of(c * CHUNK, CHUNK), CHUNK)
        att_ref[:, columns] = rows_done[:rows].astype(jnp.bfloat16)
        acc[...] += lax.dot_general(
            rows_done[rows:].astype(jnp.bfloat16), wbuf[:, columns], NT,
            preferred_element_type=jnp.float32,
        )
        return unused

    lax.fori_loop(0, CHUNKS, finish, 0, unroll=True)
    out_ref[...] = acc[...].astype(jnp.bfloat16)

    def drain(c, unused):
        for peer in peers:
            q_copy(c, me, peer).wait_send()
            p_copy(c, me, peer).wait_send()
        return unused

    lax.fori_loop(0, CHUNKS, drain, 0)


def write_out(att_ref, out_ref, att_hbm, out_hbm, sems):
    copies = [
        pltpu.make_async_copy(att_ref, att_hbm, sems.at[0]),
        pltpu.make_async_copy(out_ref, out_hbm, sems.at[1]),
    ]
    for copy in copies:
        copy.start()
    for copy in copies:
        copy.wait()


def local(
    n,
    draft_node_queries,
    draft_node_keys,
    draft_node_values,
    paged_key_cache,
    paged_value_cache,
    context_length,
    parents,
    accepted_path,
    out_weight,
):
    own = draft_node_queries.shape[0]
    rows = -(-own // 8) * 8
    if rows != own:
        pad = ((0, rows - own), (0, 0))
        draft_node_queries = jnp.pad(draft_node_queries, pad)
        draft_node_keys = jnp.pad(draft_node_keys, pad)
        draft_node_values = jnp.pad(draft_node_values, pad)
    wide = n * rows
    cached, cache_width = paged_key_cache.shape
    picked = accepted_path.shape[0]
    vmem = pl.BlockSpec(memory_space=pltpu.VMEM)
    anywhere = pl.BlockSpec(memory_space=pltpu.HBM)
    shapes = (
        jax.ShapeDtypeStruct((rows, QUERY_HEADS * HEAD_WIDTH), jnp.bfloat16),
        jax.ShapeDtypeStruct((picked, out_weight.shape[0]), jnp.bfloat16),
    )
    held = pl.pallas_call(
        functools.partial(kernel, n, own, parents.shape[0]),
        out_shape=tuple(pltpu.VMEM(shape.shape, shape.dtype) for shape in shapes),
        in_specs=[anywhere] * 9,
        out_specs=(vmem, vmem),
        scratch_shapes=[
            pltpu.SMEM(context_length.shape, jnp.int32),
            pltpu.SMEM(parents.shape, jnp.int32),
            pltpu.SMEM(accepted_path.shape, jnp.int32),
            pltpu.VMEM((rows, cache_width), jnp.bfloat16),
            pltpu.VMEM((rows, cache_width), jnp.bfloat16),
            pltpu.VMEM((CHUNKS, n, rows, CHUNK), jnp.bfloat16),
            pltpu.VMEM((cached + LANES, cache_width), jnp.bfloat16),
            pltpu.VMEM((cached + LANES, cache_width), jnp.bfloat16),
            pltpu.VMEM(out_weight.shape, jnp.bfloat16),
            pltpu.VMEM((wide, cached + LANES), jnp.float32),
            pltpu.VMEM((CHUNKS, n, rows + picked, CHUNK + LANES), jnp.bfloat16),
            pltpu.VMEM((CHUNKS, n, rows + picked, CHUNK + LANES), jnp.bfloat16),
            pltpu.VMEM((picked, out_weight.shape[0]), jnp.float32),
            pltpu.SemaphoreType.DMA((8,)),
            pltpu.SemaphoreType.DMA((CHUNKS,)),
        ]
        + [pltpu.SemaphoreType.DMA((CHUNKS, n))] * 4,
        compiler_params=pltpu.CompilerParams(
            collective_id=0, has_side_effects=True, vmem_limit_bytes=56 * 1024 * 1024
        ),
        name="verify_tree",
    )(
        context_length, parents, accepted_path,
        draft_node_queries, draft_node_keys, draft_node_values,
        paged_key_cache, paged_value_cache, out_weight,
    )
    attention, path_output = pl.pallas_call(
        write_out,
        out_shape=shapes,
        in_specs=(vmem, vmem),
        out_specs=(anywhere, anywhere),
        scratch_shapes=[pltpu.SemaphoreType.DMA((2,))],
        compiler_params=pltpu.CompilerParams(vmem_limit_bytes=1024 * 1024),
        name="write_out",
    )(*held)
    return attention[:own], path_output


def solution(mesh):
    in_specs = (
        P(("req", "blk"), None),
        P(("req", "blk"), None),
        P(("req", "blk"), None),
        P(("req", "blk"), None),
        P(("req", "blk"), None),
        P("req"),
        P("req"),
        P("req"),
        P("blk", None),
    )
    out_specs = (P(("req", "blk"), None), P("req", "blk"))
    return jax.shard_map(
        functools.partial(local, mesh.shape["blk"]),
        mesh=mesh, in_specs=in_specs, out_specs=out_specs, check_vma=False,
    )
```
